32 devices in a mesh: own: 8 (over z, x), rep: 4 (over y, core).
Axes of the slice: x: 2, y: 2, z: 4, core: 2. Of those that a mesh axis runs over, the one named last changes fastest.
Arguments:
- block_pool: bfloat16 [2048, 64, 576], P(('own', 'rep')), may hold values from -16 to 16
- sel_index: int32 [1024], P(('own', 'rep')), may hold values from 0 to 63
- sel_layer: int32 [1024], P(('own', 'rep')), may hold values from 0 to 3, as said below
- counts: int32 [32], P(('own', 'rep')), may hold values from 8 to 32, as said below
Outputs:
- quant_codes: bfloat16 [8, 4, 8, 8, 18432], P('own', 'rep')
- quant_steps: float32 [8, 288], P('own')
- clip_error: float32 [8, 288], P('own')
The draws below stay inside these ranges and needn't reach their ends.
Inputs may be any that keep to these rules, and one draw needn't show every extreme that they name: `sel_layer`: among the 32 entries of one device, at most 8 name any one layer; the first 8 entries of every device all name one and the same layer. `counts`: some device has all 32 entries live.
All inputs are finite; a program needn't handle non-finite values.
Results may differ from the reference program's by a relative error of at most 0.001.
Values may be sent and summed in bfloat16 or wider, within the bound.
A program may use at most 128 MiB of HBM per device.

```python
import math
import jax
import jax.numpy as jnp
from jax import lax

LATENT = 576
TOKB = 64
SLICES = 2
CAP = 8
POOL_DEV = 64
SEL_DEV = 32
LAYERS = 4
HALF = 288
SEL_ALL = 1024
N_OWN = 8
N_REP = 4


def draw_block_pool(key, part):
    base_key = jax.random.fold_in(key, 11)
    key_chan, key_base, key_rows = jax.random.split(base_key, 3)
    shape = (N_OWN * N_REP * POOL_DEV, TOKB, LATENT)
    channel = jnp.exp(jax.random.uniform(key_chan, (LATENT,), jnp.float32, math.log(0.3), math.log(3.0)))
    base = jnp.clip(jax.random.normal(key_base, shape, jnp.float32), -5.0, 5.0)
    row_scale = jnp.ones((shape[0], 1, 1), jnp.float32)
    return (base * channel * row_scale).astype(jnp.bfloat16)


def draw_sel_layer(key, part):
    devices = N_OWN * N_REP
    base_key = jax.random.fold_in(key, 31)
    key_star, key_perm = jax.random.split(base_key, 2)
    star_layer = jax.random.randint(key_star, (), 0, LAYERS)
    items = jnp.arange((LAYERS - 1) * CAP, dtype=jnp.int32) // CAP
    device_keys = jax.random.split(key_perm, devices)

    def per_device(device_key):
        shuffled = jax.random.permutation(device_key, items)[:SEL_DEV - CAP]
        others = (star_layer + 1 + shuffled) % LAYERS
        front = jnp.full((CAP,), star_layer, jnp.int32)
        return jnp.concatenate([front, others.astype(jnp.int32)])
    return jax.vmap(per_device)(device_keys).reshape(-1).astype(jnp.int32)


def draw_counts(key, part):
    devices = N_OWN * N_REP
    base_key = jax.random.fold_in(key, 21)
    key_low, key_full, key_first = jax.random.split(base_key, 3)
    lower = jax.random.randint(key_low, (devices,), CAP, CAP + (SEL_DEV - CAP) // 3 + 1)
    full_mask = jax.random.randint(key_full, (devices,), 0, 8) == 0
    first_full = jax.random.randint(key_first, (), 0, devices)
    full_mask = full_mask | (jnp.arange(devices) == first_full)
    return jnp.where(full_mask, SEL_DEV, lower).astype(jnp.int32)


def touch_ends(drawn, stream_key, low, high):
    index_at = [jax.random.randint(jax.random.fold_in(stream_key, axis), (), 0, length) for axis, length in enumerate(drawn.shape)]
    main_axis = drawn.shape.index(max(drawn.shape))
    neighbour = index_at[:main_axis] + [(index_at[main_axis] + 1) % drawn.shape[main_axis]] + index_at[main_axis + 1:]
    return drawn.at[tuple(index_at)].set(low).at[tuple(neighbour)].set(high)


def setup_inputs(seed: int = 0) -> dict:
    seeds = jax.random.split(jax.random.key(seed), 5)
    return {
        "block_pool": draw_block_pool(jax.random.fold_in(seeds[4], 71), 0),
        "sel_index": touch_ends(jax.random.randint(seeds[1], (SEL_ALL,), 0, POOL_DEV), jax.random.fold_in(seeds[1], 1), 0, POOL_DEV - 1).astype(jnp.int32),
        "sel_layer": draw_sel_layer(jax.random.fold_in(seeds[4], 71), 0),
        "counts": draw_counts(jax.random.fold_in(seeds[4], 71), 0),
    }


headroom = 0.5


def slot_table(index_row, layer_row, live_count, group_layer, capacity):
    n_select = index_row.shape[0]
    is_live = jnp.arange(n_select) < live_count
    matches = (layer_row[None, :] == group_layer[:, None]) & is_live[None, :]
    ranking = jnp.cumsum(matches.astype(jnp.int32), axis=1) - 1
    slot_hit = matches[:, None, :] & (ranking[:, None, :] == jnp.arange(capacity)[None, :, None])
    chosen = jnp.sum(jnp.where(slot_hit, index_row[None, None, :], 0), axis=2).astype(jnp.int32)
    filled = jnp.any(slot_hit, axis=2)
    return chosen, filled


def reference(block_pool, sel_index, sel_layer, counts):
    devices = N_OWN * N_REP
    group_layer = (jnp.arange(N_OWN) // SLICES).astype(jnp.int32)
    index_rows = sel_index.reshape(devices, SEL_DEV)
    layer_rows = sel_layer.reshape(devices, SEL_DEV)
    chosen, filled = jax.vmap(lambda a, b, c: slot_table(a, b, c, group_layer, CAP))(index_rows, layer_rows, counts)
    pools = block_pool.reshape(devices, POOL_DEV, TOKB, SLICES, HALF)
    device_ids = jnp.arange(devices)[:, None]
    denominator = float(N_OWN * N_REP * CAP * TOKB)

    def one_group(group):
        slice_of = group % SLICES
        picked = jnp.take(chosen, group, axis=1)
        keep_mask = jnp.take(filled, group, axis=1)
        blocks = pools[device_ids, picked, :, slice_of]
        blocks = jnp.where(keep_mask[:, :, None, None], blocks, jnp.zeros((), blocks.dtype))
        values = blocks.astype(jnp.float32)
        peak_abs = jnp.max(jnp.abs(values), axis=(0, 1, 2))
        step_size = headroom * jnp.maximum(peak_abs, 1.0) / 127.0
        encoded = jnp.clip(values / step_size, -127.0, 127.0).astype(jnp.bfloat16)
        encoded = lax.optimization_barrier(encoded)
        decoded = encoded.astype(jnp.float32) * step_size
        sq_error = jnp.sum((values - decoded) ** 2, axis=(0, 1, 2))
        error_out = sq_error / (step_size * step_size * denominator)
        codes_out = encoded.reshape(N_OWN, N_REP, CAP, TOKB * HALF).transpose(1, 0, 2, 3)
        return codes_out, step_size, error_out

    quant_codes, quant_steps, clip_error = lax.map(one_group, jnp.arange(N_OWN))
    return quant_codes, quant_steps, clip_error
```

```python
import functools
import math

import jax
import jax.numpy as jnp
from jax import lax
from jax.experimental import pallas as pl
from jax.experimental.pallas import tpu as pltpu
from jax.sharding import PartitionSpec as P

SLICES = 2
LANES = 128
headroom = 0.5


def slot_table(index_row, layer_row, live_count, group_layer, capacity, empty):
    n_select = index_row.shape[0]
    is_live = jnp.arange(n_select) < live_count
    matches = (layer_row[None, :] == group_layer[:, None]) & is_live[None, :]
    earlier = jnp.arange(n_select)[:, None] < jnp.arange(n_select)[None, :]
    ranking = jnp.sum((matches[:, :, None] & earlier[None]).astype(jnp.int32), axis=1)
    slot_hit = matches[:, None, :] & (ranking[:, None, :] == jnp.arange(capacity)[None, :, None])
    chosen = jnp.sum(jnp.where(slot_hit, index_row[None, None, :] - empty, 0), axis=2)
    return chosen + empty


def layer_order(layers):
    half = layers // 2
    return sorted(range(layers), key=lambda k: (k == 0, abs(k - half)))


def kernel(own_n, rep_n, cap, slot_ref, pool_ref, codes_ref, steps_ref, err_ref,
           pool_v, stage, send, recv, coded, pk_send, pk_recv, pk_mine, pk_rep, er_mine, er_rep,
           pool_sem, ssem, rsem, pssem, prsem, rpssem, rprsem, ressem, rersem, out_sem):
    rows, tokens, width = pool_ref.shape
    half = width // SLICES
    flat = tokens * half
    group = LANES // math.gcd(half, LANES)
    period = group * half
    layers = own_n // SLICES
    me = lax.axis_index("own")
    rep = lax.axis_index("rep")
    my_layer = me // SLICES
    my_slice = me % SLICES
    tiles = stage.shape[0]
    denominator = float(own_n * rep_n * cap * tokens)
    pieces = pool_sem.shape[0]
    per_piece = rows // pieces

    loads = [
        pltpu.make_async_copy(
            pool_ref.at[pl.ds(p * per_piece, per_piece)],
            pool_v.at[pl.ds(p * per_piece, per_piece)],
            pool_sem.at[p],
        )
        for p in range(pieces)
    ]
    for load in loads:
        load.start()

    barrier = pltpu.get_barrier_semaphore()
    for k in range(1, own_n):
        pl.semaphore_signal(barrier, inc=1, device_id={"own": lax.rem(me + k, own_n)},
                            device_id_type=pl.DeviceIdType.MESH)
    for k in range(1, rep_n):
        pl.semaphore_signal(barrier, inc=1, device_id={"rep": lax.rem(rep + k, rep_n)},
                            device_id_type=pl.DeviceIdType.MESH)

    pool_v[rows] = jnp.zeros((tokens, width), pool_v.dtype)
    for load in loads:
        load.wait()

    def layer_peak(layer, carry):
        best = jnp.zeros((tokens, width), pool_v.dtype)
        for c in range(cap):
            best = jnp.maximum(best, jnp.abs(pool_v[slot_ref[layer * cap + c]]))
        top = jnp.max(best.astype(jnp.float32), axis=0, keepdims=True)
        for part in range(SLICES):
            one = top[:, part * half:(part + 1) * half]
            pk_send[layer * SLICES + part] = jnp.concatenate([one] * group, axis=1)
        return carry

    lax.fori_loop(0, layers, layer_peak, 0)
    pl.semaphore_wait(barrier, own_n - 1 + rep_n - 1)

    def peak_copy(peer, landing):
        return pltpu.make_async_remote_copy(
            src_ref=pk_send.at[peer], dst_ref=pk_recv.at[landing],
            send_sem=pssem.at[peer], recv_sem=prsem.at[landing],
            device_id={"own": peer}, device_id_type=pl.DeviceIdType.MESH)

    def block_copy(peer, landing):
        return pltpu.make_async_remote_copy(
            src_ref=send.at[peer], dst_ref=recv.at[landing],
            send_sem=ssem.at[peer], recv_sem=rsem.at[landing],
            device_id={"own": peer}, device_id_type=pl.DeviceIdType.MESH)

    for k in range(1, own_n):
        peer = lax.rem(me + k, own_n)
        peak_copy(peer, me).start()

    for off in layer_order(layers):
        layer = lax.rem(my_layer + off, layers)
        for c in range(cap):
            block = pool_v[slot_ref[layer * cap + c]].astype(jnp.float32)
            for q in range(tiles):
                lo, hi = q * LANES, min(width, (q + 1) * LANES)
                stage[q, c * tokens:(c + 1) * tokens, 0:hi - lo] = block[:, lo:hi]

        def flatten(i, carry):
            rows_of = [
                jnp.concatenate(
                    [stage[q, pl.ds(i * group + j, cap, stride=tokens), :] for q in range(tiles)], axis=1)
                for j in range(group)
            ]
            for part in range(SLICES):
                joined = jnp.concatenate([r[:, part * half:(part + 1) * half] for r in rows_of], axis=1)
                at = pl.multiple_of(i * period, period)
                send[layer * SLICES + part, :, pl.ds(at, period)] = joined.astype(send.dtype)
            return carry

        lax.fori_loop(0, tokens // group, flatten, 0)
        if off:
            for part in range(SLICES):
                block_copy(layer * SLICES + part, me).start()
        else:
            for k in range(1, SLICES):
                block_copy(layer * SLICES + lax.rem(my_slice + k, SLICES), me).start()

    best = pk_send[me]
    for k in range(1, own_n):
        src = lax.rem(me + k, own_n)
        peak_copy(src, src).wait_recv()
        best = jnp.maximum(best, pk_recv[src])
    pk_mine[...] = best

    def rep_copy(mine, table, s_sem, r_sem, peer, landing):
        return pltpu.make_async_remote_copy(
            src_ref=mine, dst_ref=table.at[landing],
            send_sem=s_sem.at[peer], recv_sem=r_sem.at[landing],
            device_id={"rep": peer}, device_id_type=pl.DeviceIdType.MESH)

    for k in range(1, rep_n):
        rep_copy(pk_mine, pk_rep, rpssem, rprsem, lax.rem(rep + k, rep_n), rep).start()
    for k in range(1, rep_n):
        src = lax.rem(rep + k, rep_n)
        rep_copy(pk_mine, pk_rep, rpssem, rprsem, src, src).wait_recv()
        best = jnp.maximum(best, pk_rep[src])

    step = headroom * jnp.maximum(best, 1.0) / 127.0
    inverse = 1.0 / step
    steps_ref[...] = step[:, :half]
    step_wide = jnp.broadcast_to(step, (cap, period))
    inv_wide = jnp.broadcast_to(inverse, (cap, period))

    def out_copy(src):
        return pltpu.make_async_copy(coded.at[src], codes_ref.at[0, 0, src], out_sem.at[src])

    def encode(source, src, total):
        def one(i, total):
            at = pl.multiple_of(i * period, period)
            x = source[src, :, pl.ds(at, period)].astype(jnp.float32)
            y = jnp.clip(x * inv_wide, -127.0, 127.0).astype(coded.dtype)
            coded[src, :, pl.ds(at, period)] = y
            diff = x - y.astype(jnp.float32) * step_wide
            return total + diff * diff
        total = lax.fori_loop(0, tokens // group, one, total)
        out_copy(src).start()
        return total

    total = encode(send, me, jnp.zeros((cap, period), jnp.float32))
    for part in range(1, SLICES):
        src = my_layer * SLICES + lax.rem(my_slice + part, SLICES)
        block_copy(src, src).wait_recv()
        total = encode(recv, src, total)
    for off in layer_order(layers)[::-1][1:]:
        layer = lax.rem(my_layer - off + layers, layers)
        for part in range(SLICES):
            src = layer * SLICES + part
            block_copy(src, src).wait_recv()
            total = encode(recv, src, total)

    mine = jnp.sum(total, axis=0, keepdims=True)
    er_mine[...] = mine
    for k in range(1, rep_n):
        rep_copy(er_mine, er_rep, ressem, rersem, lax.rem(rep + k, rep_n), rep).start()
    er_rep[rep] = mine
    for k in range(1, rep_n):
        src = lax.rem(rep + k, rep_n)
        rep_copy(er_mine, er_rep, ressem, rersem, src, src).wait_recv()
    whole = er_rep[0]
    for k in range(1, rep_n):
        whole = whole + er_rep[k]
    folded = whole[:, :half]
    for j in range(1, group):
        folded = folded + whole[:, j * half:(j + 1) * half]
    narrow = step[:, :half]
    err_ref[...] = folded / (narrow * narrow * denominator)

    for k in range(1, own_n):
        peer = lax.rem(me + k, own_n)
        peak_copy(peer, me).wait_send()
        block_copy(peer, me).wait_send()
    for k in range(1, rep_n):
        peer = lax.rem(rep + k, rep_n)
        rep_copy(pk_mine, pk_rep, rpssem, rprsem, peer, rep).wait_send()
        rep_copy(er_mine, er_rep, ressem, rersem, peer, rep).wait_send()
    for src in range(own_n):
        out_copy(src).wait()


def body(block_pool, sel_index, sel_layer, counts):
    own_n = lax.axis_size("own")
    rep_n = lax.axis_size("rep")
    cap = sel_index.shape[0] // 4
    rows, tokens, width = block_pool.shape
    half = width // SLICES
    flat = tokens * half
    group = LANES // math.gcd(half, LANES)
    period = group * half
    layers = own_n // SLICES
    slots = slot_table(sel_index, sel_layer, counts[0], jnp.arange(layers), cap, rows).reshape(-1)
    f32 = jnp.float32
    dma = pltpu.SemaphoreType.DMA
    dtype = block_pool.dtype
    codes, steps, err = pl.pallas_call(
        functools.partial(kernel, own_n, rep_n, cap),
        out_shape=(
            jax.ShapeDtypeStruct((1, 1, own_n, cap, flat), dtype),
            jax.ShapeDtypeStruct((1, half), f32),
            jax.ShapeDtypeStruct((1, half), f32),
        ),
        in_specs=[pl.BlockSpec(memory_space=pltpu.SMEM), pl.BlockSpec(memory_space=pl.ANY)],
        out_specs=(
            pl.BlockSpec(memory_space=pl.ANY),
            pl.BlockSpec(memory_space=pltpu.VMEM),
            pl.BlockSpec(memory_space=pltpu.VMEM),
        ),
        scratch_shapes=[
            pltpu.VMEM((rows + 1, tokens, width), dtype),
            pltpu.VMEM((pl.cdiv(width, LANES), cap * tokens, LANES), f32),
            pltpu.VMEM((own_n, cap, flat), dtype),
            pltpu.VMEM((own_n, cap, flat), dtype),
            pltpu.VMEM((own_n, cap, flat), dtype),
            pltpu.VMEM((own_n, 1, period), f32),
            pltpu.VMEM((own_n, 1, period), f32),
            pltpu.VMEM((1, period), f32),
            pltpu.VMEM((rep_n, 1, period), f32),
            pltpu.VMEM((1, period), f32),
            pltpu.VMEM((rep_n, 1, period), f32),
            dma((8,)),
            dma((own_n,)), dma((own_n,)), dma((own_n,)), dma((own_n,)),
            dma((rep_n,)), dma((rep_n,)), dma((rep_n,)), dma((rep_n,)),
            dma((own_n,)),
        ],
        compiler_params=pltpu.CompilerParams(
            collective_id=0, has_side_effects=True, vmem_limit_bytes=60 * 1024 * 1024),
        name="latent_code",
    )(slots, block_pool)
    return codes, steps, err


def solution(mesh):
    return jax.shard_map(
        body,
        mesh=mesh,
        in_specs=(
            P(("own", "rep"), None, None),
            P(("own", "rep")),
            P(("own", "rep")),
            P(("own", "rep")),
        ),
        out_specs=(P("own", "rep", None, None, None), P("own", None), P("own", None)),
        check_vma=False,
    )
```

```python
import functools
import math

import jax
import jax.numpy as jnp
from jax import lax
from jax.experimental import pallas as pl
from jax.experimental.pallas import tpu as pltpu
from jax.sharding import PartitionSpec as P

SLICES = 2
LANES = 128
headroom = 0.5


def slot_table(index_row, layer_row, live_count, group_layer, capacity, empty):
    n_select = index_row.shape[0]
    is_live = jnp.arange(n_select) < live_count
    matches = (layer_row[None, :] == group_layer[:, None]) & is_live[None, :]
    earlier = jnp.arange(n_select)[:, None] < jnp.arange(n_select)[None, :]
    ranking = jnp.sum((matches[:, :, None] & earlier[None]).astype(jnp.int32), axis=1)
    slot_hit = matches[:, None, :] & (ranking[:, None, :] == jnp.arange(capacity)[None, :, None])
    chosen = jnp.sum(jnp.where(slot_hit, index_row[None, None, :] - empty, 0), axis=2)
    return chosen + empty


def partner_layer(my_layer, layers, k):
    near = layers // 2
    if k < near:
        return lax.rem(my_layer + k, near) + (1 - my_layer // near) * near
    return lax.rem(my_layer + 1 + k - near, near) + (my_layer // near) * near


def kernel(own_n, rep_n, cap, slot_ref, pool_ref, codes_ref, steps_ref, err_ref,
           pool_v, stage, send, recv, pk_send, pk_recv, pk_mine, pk_rep, er_mine, er_rep,
           pool_sem, ssem, rsem, pssem, prsem, rpssem, rprsem, ressem, rersem):
    rows, tokens, width = pool_ref.shape
    half = width // SLICES
    flat = tokens * half
    group = LANES // math.gcd(half, LANES)
    period = group * half
    layers = own_n // SLICES
    me = lax.axis_index("own")
    rep = lax.axis_index("rep")
    my_layer = me // SLICES
    my_slice = me % SLICES
    tiles = stage.shape[0]
    denominator = float(own_n * rep_n * cap * tokens)
    pieces = pool_sem.shape[0]
    per_piece = rows // pieces

    loads = [
        pltpu.make_async_copy(
            pool_ref.at[pl.ds(p * per_piece, per_piece)],
            pool_v.at[pl.ds(p * per_piece, per_piece)],
            pool_sem.at[p],
        )
        for p in range(pieces)
    ]
    for load in loads:
        load.start()

    barrier = pltpu.get_barrier_semaphore()
    for k in range(1, own_n):
        pl.semaphore_signal(barrier, inc=1, device_id={"own": lax.rem(me + k, own_n)},
                            device_id_type=pl.DeviceIdType.MESH)
    for k in range(1, rep_n):
        pl.semaphore_signal(barrier, inc=1, device_id={"rep": lax.rem(rep + k, rep_n)},
                            device_id_type=pl.DeviceIdType.MESH)

    pool_v[rows] = jnp.zeros((tokens, width), pool_v.dtype)
    for load in loads:
        load.wait()

    def layer_peak(layer, carry):
        best = jnp.zeros((tokens, width), pool_v.dtype)
        for c in range(cap):
            best = jnp.maximum(best, jnp.abs(pool_v[slot_ref[layer * cap + c]]))
        top = jnp.max(best.astype(jnp.float32), axis=0, keepdims=True)
        for part in range(SLICES):
            one = top[:, part * half:(part + 1) * half]
            pk_send[layer * SLICES + part] = jnp.concatenate([one] * group, axis=1)
        return carry

    lax.fori_loop(0, layers, layer_peak, 0)
    pl.semaphore_wait(barrier, own_n - 1 + rep_n - 1)

    def peak_copy(peer, landing):
        return pltpu.make_async_remote_copy(
            src_ref=pk_send.at[peer], dst_ref=pk_recv.at[landing],
            send_sem=pssem.at[peer], recv_sem=prsem.at[landing],
            device_id={"own": peer}, device_id_type=pl.DeviceIdType.MESH)

    def block_copy(peer, landing):
        return pltpu.make_async_remote_copy(
            src_ref=send.at[peer], dst_ref=recv.at[landing],
            send_sem=ssem.at[peer], recv_sem=rsem.at[landing],
            device_id={"own": peer}, device_id_type=pl.DeviceIdType.MESH)

    for k in range(1, own_n):
        peer = lax.rem(me + k, own_n)
        peak_copy(peer, me).start()

    for k in range(layers):
        layer = partner_layer(my_layer, layers, k)
        for c in range(cap):
            block = pool_v[slot_ref[layer * cap + c]].astype(jnp.float32)
            for q in range(tiles):
                lo, hi = q * LANES, min(width, (q + 1) * LANES)
                stage[q, c * tokens:(c + 1) * tokens, 0:hi - lo] = block[:, lo:hi]

        def flatten(i, carry):
            rows_of = [
                jnp.concatenate(
                    [stage[q, pl.ds(i * group + j, cap, stride=tokens), :] for q in range(tiles)], axis=1)
                for j in range(group)
            ]
            for part in range(SLICES):
                joined = jnp.concatenate([r[:, part * half:(part + 1) * half] for r in rows_of], axis=1)
                at = pl.multiple_of(i * period, period)
                send[layer * SLICES + part, :, pl.ds(at, period)] = joined.astype(send.dtype)
            return carry

        lax.fori_loop(0, tokens // group, flatten, 0)
        for part in range(1 if k == layers - 1 else 0, SLICES):
            block_copy(layer * SLICES + lax.rem(my_slice + part, SLICES), me).start()

    best = pk_send[me]
    for k in range(1, own_n):
        src = lax.rem(me + k, own_n)
        peak_copy(src, src).wait_recv()
        best = jnp.maximum(best, pk_recv[src])
    pk_mine[...] = best

    def rep_copy(mine, table, s_sem, r_sem, peer, landing):
        return pltpu.make_async_remote_copy(
            src_ref=mine, dst_ref=table.at[landing],
            send_sem=s_sem.at[peer], recv_sem=r_sem.at[landing],
            device_id={"rep": peer}, device_id_type=pl.DeviceIdType.MESH)

    for k in range(1, rep_n):
        rep_copy(pk_mine, pk_rep, rpssem, rprsem, lax.rem(rep + k, rep_n), rep).start()
    for k in range(1, rep_n):
        src = lax.rem(rep + k, rep_n)
        rep_copy(pk_mine, pk_rep, rpssem, rprsem, src, src).wait_recv()
        best = jnp.maximum(best, pk_rep[src])

    step = headroom * jnp.maximum(best, 1.0) / 127.0
    inverse = 1.0 / step
    steps_ref[...] = step[:, :half]
    step_wide = jnp.broadcast_to(step, (cap, period))
    inv_wide = jnp.broadcast_to(inverse, (cap, period))

    def encode(source, src, total):
        def one(i, total):
            at = pl.multiple_of(i * period, period)
            x = source[src, :, pl.ds(at, period)].astype(jnp.float32)
            y = jnp.clip(x * inv_wide, -127.0, 127.0).astype(codes_ref.dtype)
            codes_ref[0, 0, src, :, pl.ds(at, period)] = y
            diff = x - y.astype(jnp.float32) * step_wide
            return total + diff * diff
        return lax.fori_loop(0, tokens // group, one, total)

    total = encode(send, me, jnp.zeros((cap, period), jnp.float32))
    for part in range(1, SLICES):
        src = my_layer * SLICES + lax.rem(my_slice + part, SLICES)
        block_copy(src, src).wait_recv()
        total = encode(recv, src, total)
    for k in list(range(layers // 2, layers - 1)) + list(range(layers // 2)):
        layer = partner_layer(my_layer, layers, k)
        for part in range(SLICES):
            src = layer * SLICES + lax.rem(my_slice + part, SLICES)
            block_copy(src, src).wait_recv()
            total = encode(recv, src, total)

    mine = jnp.sum(total, axis=0, keepdims=True)
    er_mine[...] = mine
    for k in range(1, rep_n):
        rep_copy(er_mine, er_rep, ressem, rersem, lax.rem(rep + k, rep_n), rep).start()
    er_rep[rep] = mine
    for k in range(1, rep_n):
        src = lax.rem(rep + k, rep_n)
        rep_copy(er_mine, er_rep, ressem, rersem, src, src).wait_recv()
    whole = er_rep[0]
    for k in range(1, rep_n):
        whole = whole + er_rep[k]
    folded = whole[:, :half]
    for j in range(1, group):
        folded = folded + whole[:, j * half:(j + 1) * half]
    narrow = step[:, :half]
    err_ref[...] = folded / (narrow * narrow * denominator)

    for k in range(1, own_n):
        peer = lax.rem(me + k, own_n)
        peak_copy(peer, me).wait_send()
        block_copy(peer, me).wait_send()
    for k in range(1, rep_n):
        peer = lax.rem(rep + k, rep_n)
        rep_copy(pk_mine, pk_rep, rpssem, rprsem, peer, rep).wait_send()
        rep_copy(er_mine, er_rep, ressem, rersem, peer, rep).wait_send()


def body(block_pool, sel_index, sel_layer, counts):
    own_n = lax.axis_size("own")
    rep_n = lax.axis_size("rep")
    cap = sel_index.shape[0] // 4
    rows, tokens, width = block_pool.shape
    half = width // SLICES
    flat = tokens * half
    group = LANES // math.gcd(half, LANES)
    period = group * half
    layers = own_n // SLICES
    slots = slot_table(sel_index, sel_layer, counts[0], jnp.arange(layers), cap, rows).reshape(-1)
    f32 = jnp.float32
    dma = pltpu.SemaphoreType.DMA
    dtype = block_pool.dtype
    codes, steps, err = pl.pallas_call(
        functools.partial(kernel, own_n, rep_n, cap),
        out_shape=(
            pltpu.VMEM((1, 1, own_n, cap, flat), dtype),
            jax.ShapeDtypeStruct((1, half), f32),
            jax.ShapeDtypeStruct((1, half), f32),
        ),
        in_specs=[pl.BlockSpec(memory_space=pltpu.SMEM), pl.BlockSpec(memory_space=pltpu.HBM)],
        out_specs=(
            pl.BlockSpec(memory_space=pltpu.VMEM),
            pl.BlockSpec(memory_space=pltpu.VMEM),
            pl.BlockSpec(memory_space=pltpu.VMEM),
        ),
        scratch_shapes=[
            pltpu.VMEM((rows + 1, tokens, width), dtype),
            pltpu.VMEM((pl.cdiv(width, LANES), cap * tokens, LANES), f32),
            pltpu.VMEM((own_n, cap, flat), dtype),
            pltpu.VMEM((own_n, cap, flat), dtype),
            pltpu.VMEM((own_n, 1, period), f32),
            pltpu.VMEM((own_n, 1, period), f32),
            pltpu.VMEM((1, period), f32),
            pltpu.VMEM((rep_n, 1, period), f32),
            pltpu.VMEM((1, period), f32),
            pltpu.VMEM((rep_n, 1, period), f32),
            dma((8,)),
            dma((own_n,)), dma((own_n,)), dma((own_n,)), dma((own_n,)),
            dma((rep_n,)), dma((rep_n,)), dma((rep_n,)), dma((rep_n,)),
        ],
        compiler_params=pltpu.CompilerParams(
            collective_id=0, has_side_effects=True, vmem_limit_bytes=36 * 1024 * 1024),
        name="latent_code",
    )(slots, block_pool)
    return codes, steps, err


def solution(mesh):
    return jax.shard_map(
        body,
        mesh=mesh,
        in_specs=(
            P(("own", "rep"), None, None),
            P(("own", "rep")),
            P(("own", "rep")),
            P(("own", "rep")),
        ),
        out_specs=(P("own", "rep", None, None, None), P("own", None), P("own", None)),
        check_vma=False,
    )
```

```python
import functools
import math

import jax
import jax.numpy as jnp
from jax import lax
from jax.experimental import pallas as pl
from jax.experimental.pallas import tpu as pltpu
from jax.sharding import PartitionSpec as P

SLICES = 2
LANES = 128
headroom = 0.5


def partner_layer(my_layer, layers, k):
    near = layers // 2
    if k < near:
        return lax.rem(my_layer + k, near) + (1 - my_layer // near) * near
    return lax.rem(my_layer + 1 + k - near, near) + (my_layer // near) * near


def fill_slots(live, index_row, layer_row, table, layers, cap, empty):
    n_select = index_row.shape[1]
    is_live = lax.broadcasted_iota(jnp.int32, (1, n_select), 1) < live
    before = lax.broadcasted_iota(jnp.int32, (n_select, n_select), 0)
    after = lax.broadcasted_iota(jnp.int32, (n_select, n_select), 1)
    earlier = jnp.where(before < after, 1.0, 0.0)
    wanted = lax.broadcasted_iota(jnp.int32, (layers, n_select), 0)
    matches = jnp.where((layer_row == wanted) & is_live, 1.0, 0.0)
    ranking = jnp.dot(matches, earlier, preferred_element_type=jnp.float32)
    slot = lax.broadcasted_iota(jnp.int32, (cap, n_select), 0).astype(jnp.float32)
    shifted = index_row.astype(jnp.float32) - float(empty)
    for layer in range(layers):
        hit = (ranking[layer:layer + 1] == slot) & (matches[layer:layer + 1] > 0.5)
        found = jnp.sum(jnp.where(hit, shifted, 0.0), axis=1, keepdims=True) + float(empty)
        table[layer * cap:(layer + 1) * cap, :] = jnp.broadcast_to(found, (cap, LANES)).astype(jnp.int32)


def kernel(own_n, rep_n, cap, live_ref, index_ref, layer_ref, pool_ref, codes_ref, steps_ref, err_ref,
           table, slots, pool_v, stage, send, recv, pk_send, pk_recv, pk_mine, pk_rep, er_mine, er_rep,
           table_sem, pool_sem, ssem, rsem, pssem, prsem, rpssem, rprsem, ressem, rersem):
    rows, tokens, width = pool_ref.shape
    half = width // SLICES
    flat = tokens * half
    group = LANES // math.gcd(half, LANES)
    period = group * half
    layers = own_n // SLICES
    me = lax.axis_index("own")
    rep = lax.axis_index("rep")
    my_layer = me // SLICES
    my_slice = me % SLICES
    tiles = stage.shape[0]
    denominator = float(own_n * rep_n * cap * tokens)
    pieces = pool_sem.shape[0]
    per_piece = rows // pieces

    loads = [
        pltpu.make_async_copy(
            pool_ref.at[pl.ds(p * per_piece, per_piece)],
            pool_v.at[pl.ds(p * per_piece, per_piece)],
            pool_sem.at[p],
        )
        for p in range(pieces)
    ]
    for load in loads:
        load.start()

    barrier = pltpu.get_barrier_semaphore()
    for k in range(1, own_n):
        pl.semaphore_signal(barrier, inc=1, device_id={"own": lax.rem(me + k, own_n)},
                            device_id_type=pl.DeviceIdType.MESH)
    for k in range(1, rep_n):
        pl.semaphore_signal(barrier, inc=1, device_id={"rep": lax.rem(rep + k, rep_n)},
                            device_id_type=pl.DeviceIdType.MESH)

    pool_v[rows] = jnp.zeros((tokens, width), pool_v.dtype)
    fill_slots(live_ref[0], index_ref[...], layer_ref[...], table, layers, cap, rows)
    to_scalars = pltpu.make_async_copy(table, slots, table_sem)
    to_scalars.start()
    to_scalars.wait()
    for load in loads:
        load.wait()

    def row_of(slot):
        return jnp.minimum(jnp.maximum(slots[slot, 0], 0), rows)

    def layer_peak(layer, carry):
        best = jnp.zeros((tokens, width), pool_v.dtype)
        for c in range(cap):
            best = jnp.maximum(best, jnp.abs(pool_v[row_of(layer * cap + c)]))
        top = jnp.max(best.astype(jnp.float32), axis=0, keepdims=True)
        for part in range(SLICES):
            one = top[:, part * half:(part + 1) * half]
            pk_send[layer * SLICES + part] = jnp.concatenate([one] * group, axis=1)
        return carry

    def peak_copy(peer, landing):
        return pltpu.make_async_remote_copy(
            src_ref=pk_send.at[peer], dst_ref=pk_recv.at[landing],
            send_sem=pssem.at[peer], recv_sem=prsem.at[landing],
            device_id={"own": peer}, device_id_type=pl.DeviceIdType.MESH)

    def block_copy(peer, landing):
        return pltpu.make_async_remote_copy(
            src_ref=send.at[peer], dst_ref=recv.at[landing],
            send_sem=ssem.at[peer], recv_sem=rsem.at[landing],
            device_id={"own": peer}, device_id_type=pl.DeviceIdType.MESH)

    def flatten_layer(layer):
        for c in range(cap):
            block = pool_v[row_of(layer * cap + c)].astype(jnp.float32)
            for q in range(tiles):
                lo, hi = q * LANES, min(width, (q + 1) * LANES)
                stage[q, c * tokens:(c + 1) * tokens, 0:hi - lo] = block[:, lo:hi]

        def flatten(i, carry):
            rows_of = [
                jnp.concatenate(
                    [stage[q, pl.ds(i * group + j, cap, stride=tokens), :] for q in range(tiles)], axis=1)
                for j in range(group)
            ]
            for part in range(SLICES):
                joined = jnp.concatenate([r[:, part * half:(part + 1) * half] for r in rows_of], axis=1)
                at = pl.multiple_of(i * period, period)
                send[layer * SLICES + part, :, pl.ds(at, period)] = joined.astype(send.dtype)
            return carry

        lax.fori_loop(0, tokens // group, flatten, 0)

    def start_blocks(layer, parts):
        for part in parts:
            block_copy(layer * SLICES + lax.rem(my_slice + part, SLICES), me).start()

    straight, across = range(1), range(1, SLICES)
    first_far = partner_layer(my_layer, layers, 0)
    flatten_layer(first_far)
    pl.semaphore_wait(barrier, own_n - 1 + rep_n - 1)
    start_blocks(first_far, straight)

    lax.fori_loop(0, layers, layer_peak, 0)
    for k in range(1, own_n):
        peer = lax.rem(me + k, own_n)
        peak_copy(peer, me).start()

    flatten_layer(my_layer)
    start_blocks(my_layer, across)
    for k in range(layers // 2, layers - 1):
        layer = partner_layer(my_layer, layers, k)
        flatten_layer(layer)
        start_blocks(layer, range(SLICES))
    start_blocks(first_far, across)
    for k in range(1, layers // 2):
        layer = partner_layer(my_layer, layers, k)
        flatten_layer(layer)
        start_blocks(layer, range(SLICES))

    best = pk_send[me]
    for k in range(1, own_n):
        src = lax.rem(me + k, own_n)
        peak_copy(src, src).wait_recv()
        best = jnp.maximum(best, pk_recv[src])
    pk_mine[...] = best

    def rep_copy(mine, table, s_sem, r_sem, peer, landing):
        return pltpu.make_async_remote_copy(
            src_ref=mine, dst_ref=table.at[landing],
            send_sem=s_sem.at[peer], recv_sem=r_sem.at[landing],
            device_id={"rep": peer}, device_id_type=pl.DeviceIdType.MESH)

    for k in range(1, rep_n):
        rep_copy(pk_mine, pk_rep, rpssem, rprsem, lax.rem(rep + k, rep_n), rep).start()
    for k in range(1, rep_n):
        src = lax.rem(rep + k, rep_n)
        rep_copy(pk_mine, pk_rep, rpssem, rprsem, src, src).wait_recv()
        best = jnp.maximum(best, pk_rep[src])

    step = headroom * jnp.maximum(best, 1.0) / 127.0
    inverse = 1.0 / step
    steps_ref[...] = step[:, :half]
    step_wide = jnp.broadcast_to(step, (cap, period))
    inv_wide = jnp.broadcast_to(inverse, (cap, period))

    def encode(source, src, total):
        def one(i, total):
            at = pl.multiple_of(i * period, period)
            x = source[src, :, pl.ds(at, period)].astype(jnp.float32)
            y = jnp.clip(x * inv_wide, -127.0, 127.0).astype(codes_ref.dtype)
            codes_ref[0, 0, src, :, pl.ds(at, period)] = y
            diff = x - y.astype(jnp.float32) * step_wide
            return total + diff * diff
        return lax.fori_loop(0, tokens // group, one, total)

    total = encode(send, me, jnp.zeros((cap, period), jnp.float32))
    for part in range(1, SLICES):
        src = my_layer * SLICES + lax.rem(my_slice + part, SLICES)
        block_copy(src, src).wait_recv()
        total = encode(recv, src, total)
    for k in list(range(layers // 2, layers - 1)) + list(range(layers // 2)):
        layer = partner_layer(my_layer, layers, k)
        for part in range(SLICES):
            src = layer * SLICES + lax.rem(my_slice + part, SLICES)
            block_copy(src, src).wait_recv()
            total = encode(recv, src, total)

    mine = jnp.sum(total, axis=0, keepdims=True)
    er_mine[...] = mine
    for k in range(1, rep_n):
        rep_copy(er_mine, er_rep, ressem, rersem, lax.rem(rep + k, rep_n), rep).start()
    er_rep[rep] = mine
    for k in range(1, rep_n):
        src = lax.rem(rep + k, rep_n)
        rep_copy(er_mine, er_rep, ressem, rersem, src, src).wait_recv()
    whole = er_rep[0]
    for k in range(1, rep_n):
        whole = whole + er_rep[k]
    folded = whole[:, :half]
    for j in range(1, group):
        folded = folded + whole[:, j * half:(j + 1) * half]
    narrow = step[:, :half]
    err_ref[...] = folded / (narrow * narrow * denominator)

    for k in range(1, own_n):
        peer = lax.rem(me + k, own_n)
        peak_copy(peer, me).wait_send()
        block_copy(peer, me).wait_send()
    for k in range(1, rep_n):
        peer = lax.rem(rep + k, rep_n)
        rep_copy(pk_mine, pk_rep, rpssem, rprsem, peer, rep).wait_send()
        rep_copy(er_mine, er_rep, ressem, rersem, peer, rep).wait_send()


def body(block_pool, sel_index, sel_layer, counts):
    own_n = lax.axis_size("own")
    rep_n = lax.axis_size("rep")
    cap = sel_index.shape[0] // 4
    rows, tokens, width = block_pool.shape
    half = width // SLICES
    flat = tokens * half
    group = LANES // math.gcd(half, LANES)
    period = group * half
    layers = own_n // SLICES
    f32 = jnp.float32
    dma = pltpu.SemaphoreType.DMA
    dtype = block_pool.dtype
    codes, steps, err = pl.pallas_call(
        functools.partial(kernel, own_n, rep_n, cap),
        out_shape=(
            pltpu.VMEM((1, 1, own_n, cap, flat), dtype),
            jax.ShapeDtypeStruct((1, half), f32),
            jax.ShapeDtypeStruct((1, half), f32),
        ),
        in_specs=[
            pl.BlockSpec(memory_space=pltpu.SMEM), pl.BlockSpec(memory_space=pltpu.VMEM),
            pl.BlockSpec(memory_space=pltpu.VMEM), pl.BlockSpec(memory_space=pltpu.HBM)],
        out_specs=(
            pl.BlockSpec(memory_space=pltpu.VMEM),
            pl.BlockSpec(memory_space=pltpu.VMEM),
            pl.BlockSpec(memory_space=pltpu.VMEM),
        ),
        scratch_shapes=[
            pltpu.VMEM((layers * cap, LANES), jnp.int32),
            pltpu.SMEM((layers * cap, LANES), jnp.int32),
            pltpu.VMEM((rows + 1, tokens, width), dtype),
            pltpu.VMEM((pl.cdiv(width, LANES), cap * tokens, LANES), f32),
            pltpu.VMEM((own_n, cap, flat), dtype),
            pltpu.VMEM((own_n, cap, flat), dtype),
            pltpu.VMEM((own_n, 1, period), f32),
            pltpu.VMEM((own_n, 1, period), f32),
            pltpu.VMEM((1, period), f32),
            pltpu.VMEM((rep_n, 1, period), f32),
            pltpu.VMEM((1, period), f32),
            pltpu.VMEM((rep_n, 1, period), f32),
            dma, dma((8,)),
            dma((own_n,)), dma((own_n,)), dma((own_n,)), dma((own_n,)),
            dma((rep_n,)), dma((rep_n,)), dma((rep_n,)), dma((rep_n,)),
        ],
        compiler_params=pltpu.CompilerParams(
            collective_id=0, has_side_effects=True, vmem_limit_bytes=(63 * 1024 * 1024 - own_n * cap * flat * 2)),
        name="latent_code",
    )(counts, sel_index[None], sel_layer[None], block_pool)
    return codes, steps, err


def solution(mesh):
    return jax.shard_map(
        body,
        mesh=mesh,
        in_specs=(
            P(("own", "rep"), None, None),
            P(("own", "rep")),
            P(("own", "rep")),
            P(("own", "rep")),
        ),
        out_specs=(P("own", "rep", None, None, None), P("own", None), P("own", None)),
        check_vma=False,
    )
```

```python
import functools
import math

import jax
import jax.numpy as jnp
from jax import lax
from jax.experimental import pallas as pl
from jax.experimental.pallas import tpu as pltpu
from jax.sharding import PartitionSpec as P

SLICES = 2
LANES = 128
headroom = 0.5


def partner_layer(my_layer, layers, k):
    near = layers // 2
    if k < near:
        return lax.rem(my_layer + k, near) + (1 - my_layer // near) * near
    return lax.rem(my_layer + 1 + k - near, near) + (my_layer // near) * near


def send_order(layers):
    straight, across, both = range(1), range(1, SLICES), range(SLICES)
    own = [(layers - 1, across)]
    near = [(k, both) for k in range(layers // 2, layers - 1)]
    far = [(k, part) for k in range(1, layers // 2) for part in (across, straight)]
    return [(0, across), (0, straight)] + near + far + own


def fill_slots(live, index_row, layer_row, table, layers, cap, empty):
    n_select = index_row.shape[1]
    is_live = lax.broadcasted_iota(jnp.int32, (1, n_select), 1) < live
    before = lax.broadcasted_iota(jnp.int32, (n_select, n_select), 0)
    after = lax.broadcasted_iota(jnp.int32, (n_select, n_select), 1)
    earlier = jnp.where(before < after, 1.0, 0.0)
    wanted = lax.broadcasted_iota(jnp.int32, (layers, n_select), 0)
    matches = jnp.where((layer_row == wanted) & is_live, 1.0, 0.0)
    ranking = jnp.dot(matches, earlier, preferred_element_type=jnp.float32)
    slot = lax.broadcasted_iota(jnp.int32, (cap, n_select), 0).astype(jnp.float32)
    shifted = index_row.astype(jnp.float32) - float(empty)
    for layer in range(layers):
        hit = (ranking[layer:layer + 1] == slot) & (matches[layer:layer + 1] > 0.5)
        found = jnp.sum(jnp.where(hit, shifted, 0.0), axis=1, keepdims=True) + float(empty)
        table[layer * cap:(layer + 1) * cap, :] = jnp.broadcast_to(found, (cap, LANES)).astype(jnp.int32)


def kernel(own_n, rep_n, cap, live_ref, index_ref, layer_ref, pool_ref, codes_ref, steps_ref, err_ref,
           table, slots, pool_v, stage, send, recv, pk_send, pk_recv, pk_mine, pk_rep, er_mine, er_rep,
           table_sem, pool_sem, ssem, rsem, pssem, prsem, rpssem, rprsem, ressem, rersem):
    rows, tokens, width = pool_ref.shape
    half = width // SLICES
    flat = tokens * half
    group = LANES // math.gcd(half, LANES)
    period = group * half
    layers = own_n // SLICES
    me = lax.axis_index("own")
    rep = lax.axis_index("rep")
    my_layer = me // SLICES
    my_slice = me % SLICES
    tiles = stage.shape[0]
    denominator = float(own_n * rep_n * cap * tokens)
    pieces = pool_sem.shape[0]
    per_piece = rows // pieces

    loads = [
        pltpu.make_async_copy(
            pool_ref.at[pl.ds(p * per_piece, per_piece)],
            pool_v.at[pl.ds(p * per_piece, per_piece)],
            pool_sem.at[p],
        )
        for p in range(pieces)
    ]
    for load in loads:
        load.start()

    barrier = pltpu.get_barrier_semaphore()
    for k in range(1, own_n):
        pl.semaphore_signal(barrier, inc=1, device_id={"own": lax.rem(me + k, own_n)},
                            device_id_type=pl.DeviceIdType.MESH)
    for k in range(1, rep_n):
        pl.semaphore_signal(barrier, inc=1, device_id={"rep": lax.rem(rep + k, rep_n)},
                            device_id_type=pl.DeviceIdType.MESH)

    pool_v[rows] = jnp.zeros((tokens, width), pool_v.dtype)
    fill_slots(live_ref[0], index_ref[...], layer_ref[...], table, layers, cap, rows)
    to_scalars = pltpu.make_async_copy(table, slots, table_sem)
    to_scalars.start()
    to_scalars.wait()
    for load in loads:
        load.wait()

    def row_of(slot):
        return jnp.minimum(jnp.maximum(slots[slot, 0], 0), rows)

    def layer_peak(layer, carry):
        best = jnp.zeros((tokens, width), pool_v.dtype)
        for c in range(cap):
            best = jnp.maximum(best, jnp.abs(pool_v[row_of(layer * cap + c)]))
        top = jnp.max(best.astype(jnp.float32), axis=0, keepdims=True)
        for part in range(SLICES):
            one = top[:, part * half:(part + 1) * half]
            pk_send[layer * SLICES + part] = jnp.concatenate([one] * group, axis=1)
        return carry

    def peak_copy(peer, landing):
        return pltpu.make_async_remote_copy(
            src_ref=pk_send.at[peer], dst_ref=pk_recv.at[landing],
            send_sem=pssem.at[peer], recv_sem=prsem.at[landing],
            device_id={"own": peer}, device_id_type=pl.DeviceIdType.MESH)

    def block_copy(peer, landing):
        return pltpu.make_async_remote_copy(
            src_ref=send.at[peer], dst_ref=recv.at[landing],
            send_sem=ssem.at[peer], recv_sem=rsem.at[landing],
            device_id={"own": peer}, device_id_type=pl.DeviceIdType.MESH)

    def flatten_layer(layer):
        for c in range(cap):
            block = pool_v[row_of(layer * cap + c)].astype(jnp.float32)
            for q in range(tiles):
                lo, hi = q * LANES, min(width, (q + 1) * LANES)
                stage[q, c * tokens:(c + 1) * tokens, 0:hi - lo] = block[:, lo:hi]

        def flatten(i, carry):
            rows_of = [
                jnp.concatenate(
                    [stage[q, pl.ds(i * group + j, cap, stride=tokens), :] for q in range(tiles)], axis=1)
                for j in range(group)
            ]
            for part in range(SLICES):
                joined = jnp.concatenate([r[:, part * half:(part + 1) * half] for r in rows_of], axis=1)
                at = pl.multiple_of(i * period, period)
                send[layer * SLICES + part, :, pl.ds(at, period)] = joined.astype(send.dtype)
            return carry

        lax.fori_loop(0, tokens // group, flatten, 0)

    def start_blocks(layer, parts):
        for part in parts:
            block_copy(layer * SLICES + lax.rem(my_slice + part, SLICES), me).start()

    flattened = set()
    for place, (k, parts) in enumerate(send_order(layers)):
        layer = partner_layer(my_layer, layers, k)
        if k not in flattened:
            flatten_layer(layer)
            flattened.add(k)
        if not place:
            pl.semaphore_wait(barrier, own_n - 1 + rep_n - 1)
        for part in parts:
            block_copy(layer * SLICES + lax.rem(my_slice + part, SLICES), me).start()
        if place == 1:
            lax.fori_loop(0, layers, layer_peak, 0)
            for step in range(1, own_n):
                peak_copy(lax.rem(me + step, own_n), me).start()

    best = pk_send[me]
    for k in range(1, own_n):
        src = lax.rem(me + k, own_n)
        peak_copy(src, src).wait_recv()
        best = jnp.maximum(best, pk_recv[src])
    pk_mine[...] = best

    def rep_copy(mine, table, s_sem, r_sem, peer, landing):
        return pltpu.make_async_remote_copy(
            src_ref=mine, dst_ref=table.at[landing],
            send_sem=s_sem.at[peer], recv_sem=r_sem.at[landing],
            device_id={"rep": peer}, device_id_type=pl.DeviceIdType.MESH)

    for k in range(1, rep_n):
        rep_copy(pk_mine, pk_rep, rpssem, rprsem, lax.rem(rep + k, rep_n), rep).start()
    for k in range(1, rep_n):
        src = lax.rem(rep + k, rep_n)
        rep_copy(pk_mine, pk_rep, rpssem, rprsem, src, src).wait_recv()
        best = jnp.maximum(best, pk_rep[src])

    step = headroom * jnp.maximum(best, 1.0) / 127.0
    inverse = 1.0 / step
    steps_ref[...] = step[:, :half]
    step_wide = jnp.broadcast_to(step, (cap, period))
    inv_wide = jnp.broadcast_to(inverse, (cap, period))

    def encode(source, src, total):
        def one(i, total):
            at = pl.multiple_of(i * period, period)
            x = source[src, :, pl.ds(at, period)].astype(jnp.float32)
            y = jnp.clip(x * inv_wide, -127.0, 127.0).astype(codes_ref.dtype)
            codes_ref[0, 0, src, :, pl.ds(at, period)] = y
            diff = x - y.astype(jnp.float32) * step_wide
            return total + diff * diff
        return lax.fori_loop(0, tokens // group, one, total)

    total = encode(send, me, jnp.zeros((cap, period), jnp.float32))
    for part in range(1, SLICES):
        src = my_layer * SLICES + lax.rem(my_slice + part, SLICES)
        block_copy(src, src).wait_recv()
        total = encode(recv, src, total)
    for k in list(range(layers // 2, layers - 1)) + list(range(layers // 2)):
        layer = partner_layer(my_layer, layers, k)
        for part in range(SLICES):
            src = layer * SLICES + lax.rem(my_slice + part, SLICES)
            block_copy(src, src).wait_recv()
            total = encode(recv, src, total)

    mine = jnp.sum(total, axis=0, keepdims=True)
    er_mine[...] = mine
    for k in range(1, rep_n):
        rep_copy(er_mine, er_rep, ressem, rersem, lax.rem(rep + k, rep_n), rep).start()
    er_rep[rep] = mine
    for k in range(1, rep_n):
        src = lax.rem(rep + k, rep_n)
        rep_copy(er_mine, er_rep, ressem, rersem, src, src).wait_recv()
    whole = er_rep[0]
    for k in range(1, rep_n):
        whole = whole + er_rep[k]
    folded = whole[:, :half]
    for j in range(1, group):
        folded = folded + whole[:, j * half:(j + 1) * half]
    narrow = step[:, :half]
    err_ref[...] = folded / (narrow * narrow * denominator)

    for k in range(1, own_n):
        peer = lax.rem(me + k, own_n)
        peak_copy(peer, me).wait_send()
        block_copy(peer, me).wait_send()
    for k in range(1, rep_n):
        peer = lax.rem(rep + k, rep_n)
        rep_copy(pk_mine, pk_rep, rpssem, rprsem, peer, rep).wait_send()
        rep_copy(er_mine, er_rep, ressem, rersem, peer, rep).wait_send()


def write_out(codes_v, steps_v, err_v, codes_ref, steps_ref, err_ref, sems):
    own_n = codes_v.shape[2]
    moves = [pltpu.make_async_copy(codes_v.at[0, 0, src], codes_ref.at[0, 0, src], sems.at[src])
             for src in range(own_n)]
    moves.append(pltpu.make_async_copy(steps_v, steps_ref, sems.at[own_n]))
    moves.append(pltpu.make_async_copy(err_v, err_ref, sems.at[own_n + 1]))
    for move in moves:
        move.start()
    for move in moves:
        move.wait()


def body(block_pool, sel_index, sel_layer, counts):
    own_n = lax.axis_size("own")
    rep_n = lax.axis_size("rep")
    cap = sel_index.shape[0] // 4
    rows, tokens, width = block_pool.shape
    half = width // SLICES
    flat = tokens * half
    group = LANES // math.gcd(half, LANES)
    period = group * half
    layers = own_n // SLICES
    f32 = jnp.float32
    dma = pltpu.SemaphoreType.DMA
    dtype = block_pool.dtype
    codes, steps, err = pl.pallas_call(
        functools.partial(kernel, own_n, rep_n, cap),
        out_shape=(
            pltpu.VMEM((1, 1, own_n, cap, flat), dtype),
            pltpu.VMEM((1, half), f32),
            pltpu.VMEM((1, half), f32),
        ),
        in_specs=[
            pl.BlockSpec(memory_space=pltpu.SMEM), pl.BlockSpec(memory_space=pltpu.VMEM),
            pl.BlockSpec(memory_space=pltpu.VMEM), pl.BlockSpec(memory_space=pltpu.HBM)],
        out_specs=(
            pl.BlockSpec(memory_space=pltpu.VMEM),
            pl.BlockSpec(memory_space=pltpu.VMEM),
            pl.BlockSpec(memory_space=pltpu.VMEM),
        ),
        scratch_shapes=[
            pltpu.VMEM((layers * cap, LANES), jnp.int32),
            pltpu.SMEM((layers * cap, LANES), jnp.int32),
            pltpu.VMEM((rows + 1, tokens, width), dtype),
            pltpu.VMEM((pl.cdiv(width, LANES), cap * tokens, LANES), f32),
            pltpu.VMEM((own_n, cap, flat), dtype),
            pltpu.VMEM((own_n, cap, flat), dtype),
            pltpu.VMEM((own_n, 1, period), f32),
            pltpu.VMEM((own_n, 1, period), f32),
            pltpu.VMEM((1, period), f32),
            pltpu.VMEM((rep_n, 1, period), f32),
            pltpu.VMEM((1, period), f32),
            pltpu.VMEM((rep_n, 1, period), f32),
            dma, dma((8,)),
            dma((own_n,)), dma((own_n,)), dma((own_n,)), dma((own_n,)),
            dma((rep_n,)), dma((rep_n,)), dma((rep_n,)), dma((rep_n,)),
        ],
        compiler_params=pltpu.CompilerParams(
            collective_id=0, has_side_effects=True, vmem_limit_bytes=(63 * 1024 * 1024 - own_n * cap * flat * 2)),
        name="latent_code",
    )(counts, sel_index[None], sel_layer[None], block_pool)
    hbm = pl.BlockSpec(memory_space=pltpu.HBM)
    return pl.pallas_call(
        write_out,
        out_shape=tuple(jax.ShapeDtypeStruct(x.shape, x.dtype) for x in (codes, steps, err)),
        in_specs=[pl.BlockSpec(memory_space=pltpu.VMEM)] * 3,
        out_specs=(hbm, hbm, hbm),
        scratch_shapes=[dma((own_n + 2,))],
        compiler_params=pltpu.CompilerParams(vmem_limit_bytes=4 * 1024 * 1024),
        name="write_out",
    )(codes, steps, err)


def solution(mesh):
    return jax.shard_map(
        body,
        mesh=mesh,
        in_specs=(
            P(("own", "rep"), None, None),
            P(("own", "rep")),
            P(("own", "rep")),
            P(("own", "rep")),
        ),
        out_specs=(P("own", "rep", None, None, None), P("own", None), P("own", None)),
        check_vma=False,
    )
```
